32 devices in a mesh: grp: 2 (over y), row: 4 (over x, core), col: 4 (over z).
Axes of the slice: x: 2, y: 2, z: 4, core: 2. Of those that a mesh axis runs over, the one named last changes fastest.
Arguments:
- perturbation: bfloat16 [4, 12000, 12000], P('grp', 'row', 'col'), parts along dimension 0, may hold values from -96 to 96
- occ_coeffs: bfloat16 [12000, 2000], P('row', 'col'), may hold values from -0.0546875 to 0.0546875
- vir_coeffs: bfloat16 [12000, 512], P('col', 'row'), may hold values from -0.0546875 to 0.0546875
- occ_energies: float32 [2000], replicated, may hold values from -1 to -0.1
- vir_energies: float32 [512], replicated, may hold values from 0.1 to 1.5
Outputs:
- density_response: bfloat16 [4, 12000, 12000], P('grp', 'row', 'col'), parts along dimension 0
The draws below stay inside these ranges and needn't reach their ends.
There are 2 independent parts, one for each index of `grp`. The reference program is written for one: setup_inputs(seed, part) draws one part's arguments, and reference() takes and returns one part's arrays. A program takes and returns all parts, laid end to end along the dimension named above; an argument that names none is the same for every part. Nothing has to cross between parts.
All inputs are finite; a program needn't handle non-finite values.
Results may differ from the reference program's by a relative error of at most 0.0098.
Values may be sent and summed in bfloat16 or wider, within the bound.
A program may use at most 192 MiB of HBM per device.

```python
import jax
import jax.numpy as jnp
from jax import lax

NB = 12000
NOCC = 2000
NV = 512
PERT = 2


def block_levels(rng, shape, cuts, smallest, high):
    factor_of = 1.0
    for dim, shards_of in cuts:
        draws = jax.random.uniform(jax.random.fold_in(jax.random.fold_in(rng, 6), dim), (shards_of,), jnp.float32, smallest / len(cuts), high / len(cuts))
        factor_of = factor_of * jnp.repeat(jnp.exp(draws), shape[dim] // shards_of).reshape((-1,) + (1,) * (len(shape) - 1 - dim))
    return factor_of


def scatter_about(key, shape, spread, bound, cuts=(), held_as=jnp.bfloat16):
    array = spread * jax.random.normal(key, shape, jnp.float32)
    if cuts:
        array = array * block_levels(key, shape, cuts, -0.22, 0.18)
    return jnp.clip(array, -bound, bound).astype(held_as)


def setup_inputs(seed: int = 0, part: int = 0) -> dict:
    seeds = jax.random.split(jax.random.key(seed), 6)
    part_keys = jax.random.split(jax.random.fold_in(seeds[5], part), 6)
    return {
        "perturbation": scatter_about(part_keys[0], (PERT, NB, NB), 16.0, 96.0, ((1, 4), (2, 4))),
        "occ_coeffs": scatter_about(seeds[1], (NB, NOCC), NB ** -0.5, 0.0546875, ((0, 4), (1, 4))),
        "vir_coeffs": scatter_about(seeds[2], (NB, NV), NB ** -0.5, 0.0546875, ((0, 4), (1, 4))),
        "occ_energies": jnp.clip(jax.random.uniform(seeds[3], (NOCC,), jnp.float32, -1.0, -0.1), -1.0, -0.1),
        "vir_energies": jnp.clip(jax.random.uniform(seeds[4], (NV,), jnp.float32, 0.1, 1.5), 0.1, 1.5),
    }


def reference(perturbation, occ_coeffs, vir_coeffs, occ_energies, vir_energies):
    gaps = occ_energies[:, None] - vir_energies[None, :]
    occ_wide = occ_coeffs.astype(jnp.float32)
    results = []
    for index in range(PERT):
        image = jnp.dot(perturbation[index], vir_coeffs, preferred_element_type=jnp.float32)
        coupling = jnp.dot(occ_wide.T, image, precision=lax.Precision.HIGHEST)
        response = (coupling / gaps).astype(jnp.bfloat16)
        mixed = jnp.dot(occ_coeffs, response, preferred_element_type=jnp.float32).astype(jnp.bfloat16)
        results.append(jnp.dot(mixed, vir_coeffs.T, preferred_element_type=jnp.float32).astype(jnp.bfloat16))
    return jnp.stack(results)
```

```python
import functools

import jax
import jax.numpy as jnp
from jax import lax
from jax.experimental import pallas as pl
from jax.experimental.pallas import tpu as pltpu
from jax.sharding import PartitionSpec as P

BF16 = jnp.bfloat16
F32 = jnp.float32
MESH = pl.DeviceIdType.MESH
NT = (((1,), (1,)), ((), ()))
NN = (((1,), (0,)), ((), ()))
PIECES = 4


def up(value, step):
    return -(-value // step) * step


def flip(index, bit):
    return index + bit - 2 * bit * ((index // bit) % 2)


def pick(position, options):
    value = jnp.int32(0)
    for index, option in enumerate(options):
        value = value + jnp.where(position == index, jnp.int32(option), jnp.int32(0))
    return value


def arrivals(cols, position):
    order = [(position, 0), (position, 1)]
    for slot in range(cols - 1):
        blocks = [b for b in (position - 1 - slot, position + 1 + slot) if 0 <= b < cols]
        order += [(b, 0) for b in blocks] + [(b, 1) for b in blocks]
    return order


def gather_kernel(
    dims,
    h_hbm, occ_hbm, vir_hbm, occ_e, vir_e,
    mixed_hbm, virt_hbm,
    occ, virt, hbuf, image, part, rs1, rs2s, rs2r, resp, acc, stage,
    loc_sem, h_sem, vs_sem, vr_sem, zs_sem, zr_sem, ys_sem, yr_sem,
    a_s, a_r, b_s, b_r, c_s, c_r, d_s, d_r, o_sem,
):
    rows, cols = dims["rows"], dims["cols"]
    pert, ni, hb, nb = dims["pert"], dims["ni"], dims["hb"], dims["nb"]
    nv, ip, piece, wh = dims["nv"], dims["ip"], dims["piece"], dims["wh"]
    pv = pert * nv
    pr = pv // rows
    ps = pr // cols
    grp, row, col = lax.axis_index("grp"), lax.axis_index("row"), lax.axis_index("col")
    other = 1 - grp

    barrier = pltpu.get_barrier_semaphore()
    for d in range(1, rows):
        pl.semaphore_signal(barrier, inc=1, device_id={"row": (row + d) % rows}, device_id_type=MESH)
    for e in range(1, cols):
        pl.semaphore_signal(barrier, inc=1, device_id={"col": (col + e) % cols}, device_id_type=MESH)
    pl.semaphore_signal(barrier, inc=1, device_id={"grp": other}, device_id_type=MESH)

    def half_copy(half, sem):
        return pltpu.make_async_copy(
            occ_hbm.at[:, pl.ds(pl.multiple_of(half * wh, wh), wh)], occ.at[col, half], loc_sem.at[sem]
        )

    half_copy(grp, 0).start()
    vir_copy = pltpu.make_async_copy(vir_hbm, virt.at[row], loc_sem.at[2])
    vir_copy.start()
    half_copy(other, 1).start()

    def h_copy(n, act):
        p, b, slot = n // nb, n % nb, n % 2
        last = ni - (nb - 1) * hb

        def go(size):
            copy = pltpu.make_async_copy(
                h_hbm.at[p, pl.ds(pl.multiple_of(b * hb, hb), size)], hbuf.at[slot, pl.ds(0, size)], h_sem.at[slot]
            )
            act(copy)

        if nb == 1:
            act(pltpu.make_async_copy(h_hbm.at[p], hbuf.at[slot], h_sem.at[slot]))
        elif last == hb:
            go(hb)
        else:
            pl.when(b < nb - 1)(lambda: go(hb))
            pl.when(b == nb - 1)(lambda: go(last))

    h_copy(jnp.int32(0), lambda c: c.start())
    pl.semaphore_wait(barrier, rows + cols - 1)

    def vir_send(block, target, n):
        return pltpu.make_async_remote_copy(
            src_ref=virt.at[block], dst_ref=virt.at[block], send_sem=vs_sem.at[n], recv_sem=vr_sem.at[block],
            device_id={"row": target}, device_id_type=MESH,
        )

    vir_copy.wait()
    top = rows // 2
    vir_send(row, flip(row, top), 0).start()

    def z_send(block, q, target, way):
        ref = occ.at[block, grp, pl.ds(q * piece, piece)]
        return pltpu.make_async_remote_copy(
            src_ref=ref, dst_ref=ref, send_sem=zs_sem.at[way, block], recv_sem=zr_sem.at[block, q],
            device_id={"col": target}, device_id_type=MESH,
        )

    def y_send(block, q):
        ref = occ.at[block, grp, pl.ds(q * piece, piece)]
        return pltpu.make_async_remote_copy(
            src_ref=ref, dst_ref=ref, send_sem=ys_sem.at[block], recv_sem=yr_sem.at[block],
            device_id={"grp": other}, device_id_type=MESH,
        )

    half_copy(grp, 0).wait()
    for q in range(PIECES):
        pl.when(col >= 1)(lambda q=q: z_send(col, q, col - 1, 0).start())
        pl.when(col <= cols - 2)(lambda q=q: z_send(col, q, col + 1, 1).start())

    def pump(slot, q):
        def from_left():
            block = col - 1 - slot
            z_send(block, q, 0, 1).wait_recv()
            pl.when(col <= cols - 2)(lambda: z_send(block, q, col + 1, 1).start())
            y_send(block, q).start()

        def from_right():
            block = col + 1 + slot
            z_send(block, q, 0, 0).wait_recv()
            pl.when(col >= 1)(lambda: z_send(block, q, col - 1, 0).start())
            y_send(block, q).start()

        pl.when(col - 1 - slot >= 0)(from_left)
        pl.when(col + 1 + slot <= cols - 1)(from_right)

    pump(0, 0)
    held, bit = [0], top
    while bit >= 1:
        if bit != top:
            for h_at, h in enumerate(held):
                vir_send(flip_all(row, h), flip(row, bit), len(held) - 1 + h_at).start()
        for h in held:
            vir_send(flip_all(row, h + bit), row, 0).wait_recv()
        held = held + [h + bit for h in held]
        bit //= 2
    virt_out = pltpu.make_async_copy(virt, virt_hbm, loc_sem.at[2])
    virt_out.start()
    if PIECES > 1:
        pump(0, 1)

    steps = pert * nb

    def image_step(n, carry):
        pl.when(n + 1 < steps)(lambda: h_copy(n + 1, lambda c: c.start()))
        h_copy(n, lambda c: c.wait())
        p, b, slot = n // nb, n % nb, n % 2
        lhs = virt[...].reshape(nv, virt.shape[2])
        value = lax.dot_general(lhs, hbuf[slot], NT, preferred_element_type=F32)
        basis = lax.broadcasted_iota(jnp.int32, (1, hb), 1) + b * hb
        value = jnp.where(basis < ni, value, 0.0).astype(BF16)
        at = pl.ds(pl.multiple_of(p * nv, nv), nv)
        if nb == 1:
            image[at, :] = jnp.zeros((nv, ip), BF16)
            image[at, 0:hb] = value
        else:
            image[at, pl.ds(pl.multiple_of(b * hb, hb), hb)] = value
        for q in range(2, PIECES):
            at = min(steps - 1, (q - 1) * steps // (PIECES - 1))
            pl.when(n == at)(lambda q=q: pump(0, q))
        return carry

    lax.fori_loop(0, steps, image_step, 0)
    half_copy(other, 1).wait()

    order = [arrivals(cols, position) for position in range(cols)]

    def chunk(s):
        block = pick(col, [order[position][s][0] for position in range(cols)])
        second = pick(col, [order[position][s][1] for position in range(cols)])
        half = grp * (1 - second) + other * second
        return block, second, half

    def rs1_send(block, half, d, target):
        return pltpu.make_async_remote_copy(
            src_ref=part.at[block, half, target], dst_ref=rs1.at[block, half, d - 1],
            send_sem=a_s.at[block, half], recv_sem=a_r.at[block, half],
            device_id={"row": target}, device_id_type=MESH,
        )

    def make_part(s):
        block, second, half = chunk(s)
        if s >= 2:
            def await_second():
                pltpu.make_async_copy(occ.at[block, half], occ.at[block, half], yr_sem.at[block]).wait()
            pl.when(second == 1)(await_second)

        def body(d, carry):
            target = (row + d) % rows
            lhs = image[pl.ds(pl.multiple_of(target * pr, pr), pr), :]
            value = lax.dot_general(lhs, occ[block, half], NN, preferred_element_type=F32)
            part[block, half, target] = value.astype(BF16)
            pl.when(d < rows)(lambda: rs1_send(block, half, d, target).start())
            return carry

        lax.fori_loop(1, rows + 1, body, 0)

    def rs2_send(block, half, e):
        target = (col + e) % cols
        return pltpu.make_async_remote_copy(
            src_ref=rs2s.at[block, half, target], dst_ref=rs2r.at[block, half, e - 1],
            send_sem=b_s.at[block, half], recv_sem=b_r.at[block, half],
            device_id={"col": target}, device_id_type=MESH,
        )

    def combine(s):
        block, second, half = chunk(s)
        pltpu.make_async_copy(rs1.at[block, half], rs1.at[block, half], a_r.at[block, half]).wait()
        total = part[block, half, row].astype(F32)
        for d in range(rows - 1):
            total = total + rs1[block, half, d].astype(F32)
        rs2s[block, half] = total.reshape(cols, ps, wh).astype(BF16)
        for e in range(1, cols):
            rs2_send(block, half, e).start()

    def pair(d, second):
        half = grp if second == 0 else other
        return [(cols // 2 - 1 - d, half), (cols // 2 + d, half)]

    def ag1_send(block, half, e):
        ref = resp.at[block, half, row, col]
        return pltpu.make_async_remote_copy(
            src_ref=ref, dst_ref=ref, send_sem=c_s.at[block, half], recv_sem=c_r.at[block, half],
            device_id={"col": (col + e) % cols}, device_id_type=MESH,
        )

    def ag2_send(block, half, d):
        ref = resp.at[block, half, row]
        return pltpu.make_async_remote_copy(
            src_ref=ref, dst_ref=ref, send_sem=d_s.at[block, half], recv_sem=d_r.at[block, half],
            device_id={"row": (row + d) % rows}, device_id_type=MESH,
        )

    def respond(d, second):
        for block, half in pair(d, second):
            pltpu.make_async_copy(rs2r.at[block, half], rs2r.at[block, half], b_r.at[block, half]).wait()
            total = rs2s[block, half, col].astype(F32)
            for e in range(cols - 1):
                total = total + rs2r[block, half, e].astype(F32)
            gaps = occ_e[block, half] - vir_e[pl.ds(pl.multiple_of(row * pr + col * ps, ps), ps), :]
            resp[block, half, row, col] = (total / gaps).astype(BF16)
            for e in range(1, cols):
                ag1_send(block, half, e).start()

    def spread(d, second):
        for block, half in pair(d, second):
            some = resp.at[block, half, row, pl.ds(0, cols - 1)]
            pltpu.make_async_copy(some, some, c_r.at[block, half]).wait()
            for e in range(1, rows):
                ag2_send(block, half, e).start()

    tile = dims["tile"]
    tiles = ip // tile

    def out_copy(n, slot):
        return [
            pltpu.make_async_copy(
                stage.at[slot, p], mixed_hbm.at[p, pl.ds(pl.multiple_of(n * tile, tile), tile)], o_sem.at[slot]
            )
            for p in range(pert)
        ]

    def mix(d, second, first, last):
        chunks = pair(d, second)
        for block, half in chunks:
            some = resp.at[block, half, pl.ds(0, rows - 1)]
            pltpu.make_async_copy(some, some, d_r.at[block, half]).wait()

        def body(n, carry):
            at = pl.ds(pl.multiple_of(n * tile, tile), tile)
            if last:
                def free():
                    for copy in out_copy(n - 2, n % 2):
                        copy.wait()
                pl.when(n >= 2)(free)
            for p in range(pert):
                across = rows // pert
                total = None
                for block, half in chunks:
                    rhs = resp[block, half, pl.ds(p * across, across)]
                    rhs = rhs.astype(F32).reshape(nv, wh).astype(BF16)
                    value = lax.dot_general(occ[block, half, at], rhs, NT, preferred_element_type=F32)
                    total = value if total is None else total + value
                if not first:
                    total = total + acc[p, at]
                if last:
                    stage[n % 2, p] = total.astype(BF16)
                else:
                    acc[p, at] = total
            if last:
                for copy in out_copy(n, n % 2):
                    copy.start()
            return carry

        lax.fori_loop(0, tiles, body, 0)
        if last:
            for n in range(max(0, tiles - 2), tiles):
                for copy in out_copy(n, n % 2):
                    copy.wait()

    left = [(t, q) for t in range(1, cols - 1) for q in range(PIECES)]

    def through(slot):
        while left and left[0][0] <= slot:
            pump(*left.pop(0))

    def some_pumps(count, slot):
        for _ in range(count):
            if left and left[0][0] <= slot:
                pump(*left.pop(0))

    make_part(0)
    make_part(1)
    combine(0)
    make_part(2)
    combine(1)
    some_pumps(2, 1)
    make_part(3)
    combine(2)
    some_pumps(1, 1)
    combine(3)
    through(1)
    started = False
    for s in range(4, cols + 1):
        through((s - 2) // 2)
        make_part(s)
        some_pumps(1, (s - 2) // 2 + 1)
        combine(s)
    for d in range(cols // 2):
        s = cols + 2 * d
        if d > 0:
            through((s - 2) // 2)
            make_part(s)
            combine(s)
        final = d == cols // 2 - 1
        make_part(s + 1)
        respond(d, 0)
        some_pumps(1, s // 2)
        combine(s + 1)
        spread(d, 0)
        some_pumps(1, s // 2)
        respond(d, 1)
        mix(d, 0, not started, False)
        started = True
        some_pumps(1, s // 2)
        spread(d, 1)
        mix(d, 1, False, final)

    virt_out.wait()
    for n in range(rows - 1):
        vir_send(row, row, n).wait_send()
    for block in range(cols):
        whole = occ.at[block, 0]

        def sent(sem, whole=whole):
            pltpu.make_async_copy(whole, whole, sem).wait()

        pl.when((col >= 1) & (col <= block))(lambda: sent(zs_sem.at[0, block]))
        pl.when((col <= cols - 2) & (col >= block))(lambda: sent(zs_sem.at[1, block]))
        pl.when(col != block)(lambda: sent(ys_sem.at[block]))
        for half in range(2):
            sizes = (
                (a_s, rs1.at[block, half]),
                (b_s, rs2r.at[block, half]),
                (c_s, resp.at[block, half, 0, pl.ds(0, cols - 1)]),
                (d_s, resp.at[block, half, pl.ds(0, rows - 1)]),
            )
            for sem, ref in sizes:
                pltpu.make_async_copy(ref, ref, sem.at[block, half]).wait()


def flip_all(index, mask):
    bit = 1
    while bit <= mask:
        if mask & bit:
            index = flip(index, bit)
        bit *= 2
    return index


def final_kernel(mixed_ref, virt_ref, out_ref):
    out_ref[0] = lax.dot_general(mixed_ref[0], virt_ref[...], NN, preferred_element_type=F32).astype(BF16)


def per_device(mesh, perturbation, occ_coeffs, vir_coeffs, occ_energies, vir_energies):
    rows, cols = mesh.shape["row"], mesh.shape["col"]
    pert, ni, nj = perturbation.shape
    width = occ_coeffs.shape[1]
    nv = vir_coeffs.shape[1] * rows
    wh = up(-(-width // 2), 128)
    piece = up(-(-ni // PIECES), 64)
    ip = piece * PIECES
    hb = 512 if ni % 8 == 0 and ni > 512 else ni
    nb = -(-ni // hb)
    ip = up(max(nb * hb, ip), 256)
    piece = ip // PIECES
    pv = pert * nv
    pr = pv // rows
    ps = pr // cols
    tile = 512 if ip % 512 == 0 else 256
    dims = dict(rows=rows, cols=cols, pert=pert, ni=ni, hb=hb, nb=nb, nv=nv, ip=ip, piece=piece, wh=wh, tile=tile)

    occ_padded = jnp.pad(occ_coeffs, ((0, ip - ni), (0, 2 * wh - width)))
    vir_t = vir_coeffs.T
    occ_e = jnp.pad(occ_energies.reshape(cols, width), ((0, 0), (0, 2 * wh - width)), constant_values=-1.0)
    occ_e = occ_e.reshape(cols, 2, 1, wh)
    vir_e = jnp.tile(vir_energies, pert)[:, None]

    any_space = pl.BlockSpec(memory_space=pl.ANY)
    vmem = pl.BlockSpec(memory_space=pltpu.VMEM)
    dma = pltpu.SemaphoreType.DMA
    mixed, virt = pl.pallas_call(
        functools.partial(gather_kernel, dims),
        out_shape=(
            jax.ShapeDtypeStruct((pert, ip, nv), BF16),
            jax.ShapeDtypeStruct((rows, nv // rows, nj), BF16),
        ),
        in_specs=[any_space, any_space, any_space, vmem, vmem],
        out_specs=(any_space, any_space),
        scratch_shapes=[
            pltpu.VMEM((cols, 2, ip, wh), BF16),
            pltpu.VMEM((rows, nv // rows, nj), BF16),
            pltpu.VMEM((2, hb, nj), BF16),
            pltpu.VMEM((pv, ip), BF16),
            pltpu.VMEM((cols, 2, rows, pr, wh), BF16),
            pltpu.VMEM((cols, 2, rows - 1, pr, wh), BF16),
            pltpu.VMEM((cols, 2, cols, ps, wh), BF16),
            pltpu.VMEM((cols, 2, cols - 1, ps, wh), BF16),
            pltpu.VMEM((cols, 2, rows, cols, ps, wh), BF16),
            pltpu.VMEM((pert, ip, nv), F32),
            pltpu.VMEM((2, pert, tile, nv), BF16),
            dma((3,)), dma((2,)), dma((rows,)), dma((rows,)),
            dma((2, cols)), dma((cols, PIECES)), dma((cols,)), dma((cols,)),
            dma((cols, 2)), dma((cols, 2)), dma((cols, 2)), dma((cols, 2)),
            dma((cols, 2)), dma((cols, 2)), dma((cols, 2)), dma((cols, 2)),
            dma((2,)),
        ],
        compiler_params=pltpu.CompilerParams(
            collective_id=0, has_side_effects=True, vmem_limit_bytes=67043328
        ),
        name="gather",
    )(perturbation, occ_padded, vir_t, occ_e, vir_e)

    virt = virt.reshape(nv, nj)
    block = 384 if ip % 384 == 0 else 256
    return pl.pallas_call(
        final_kernel,
        out_shape=jax.ShapeDtypeStruct((pert, ni, nj), BF16),
        grid=(pert, ip // block),
        in_specs=[
            pl.BlockSpec((1, block, nv), lambda p, i: (p, i, 0)),
            pl.BlockSpec((nv, nj), lambda p, i: (0, 0)),
        ],
        out_specs=pl.BlockSpec((1, block, nj), lambda p, i: (p, i, 0)),
        compiler_params=pltpu.CompilerParams(vmem_limit_bytes=56 * 1024 * 1024),
        name="final",
    )(mixed, virt)


def solution(mesh):
    placed = (P("grp", "row", "col"), P("row", "col"), P("col", "row"), P(), P())
    return jax.shard_map(
        functools.partial(per_device, mesh), mesh=mesh, in_specs=placed,
        out_specs=P("grp", "row", "col"), check_vma=False,
    )
```

```python
import functools

import jax
import jax.numpy as jnp
from jax import lax
from jax.experimental import pallas as pl
from jax.experimental.pallas import tpu as pltpu
from jax.sharding import PartitionSpec as P

BF16 = jnp.bfloat16
F32 = jnp.float32
MESH = pl.DeviceIdType.MESH
NT = (((1,), (1,)), ((), ()))
NN = (((1,), (0,)), ((), ()))
PIECES = 4
HELD = 0


def up(value, step):
    return -(-value // step) * step


def flip(index, bit):
    return index + bit - 2 * bit * ((index // bit) % 2)


def pick(position, options):
    value = jnp.int32(0)
    for index, option in enumerate(options):
        value = value + jnp.where(position == index, jnp.int32(option), jnp.int32(0))
    return value


def arrivals(cols, position):
    order = [(position, 0), (position, 1)]
    for slot in range(cols - 1):
        blocks = [b for b in (position - 1 - slot, position + 1 + slot) if 0 <= b < cols]
        order += [(b, 0) for b in blocks] + [(b, 1) for b in blocks]
    return order


def gather_kernel(
    dims,
    h_hbm, occ_hbm, vir_hbm, occ_e, vir_e,
    mixed_hbm, virt_hbm,
    occ, virt, hbuf, image, part, rs1, rs2s, rs2r, resp, acc, stage, vraw,
    loc_sem, h_sem, vs_sem, vr_sem, zs_sem, zr_sem, ys_sem, yr_sem,
    a_s, a_r, b_s, b_r, c_s, c_r, d_s, d_r, o_sem,
):
    rows, cols = dims["rows"], dims["cols"]
    pert, ni, hb, nb = dims["pert"], dims["ni"], dims["hb"], dims["nb"]
    nv, ip, piece, wh, nr = dims["nv"], dims["ip"], dims["piece"], dims["wh"], dims["nr"]
    pv = pert * nv
    pr = pv // rows
    ps = pr // cols
    grp, row, col = lax.axis_index("grp"), lax.axis_index("row"), lax.axis_index("col")
    other = 1 - grp

    barrier = pltpu.get_barrier_semaphore()
    for d in range(1, rows):
        pl.semaphore_signal(barrier, inc=1, device_id={"row": (row + d) % rows}, device_id_type=MESH)
    for e in range(1, cols):
        pl.semaphore_signal(barrier, inc=1, device_id={"col": (col + e) % cols}, device_id_type=MESH)
    pl.semaphore_signal(barrier, inc=1, device_id={"grp": other}, device_id_type=MESH)

    def half_copy(half, sem):
        return pltpu.make_async_copy(
            occ_hbm.at[:, pl.ds(pl.multiple_of(half * wh, wh), wh)], occ.at[col, half, pl.ds(0, nr)], loc_sem.at[sem]
        )

    def rows_of(q):
        return pl.ds(q * piece, min(piece, nr - q * piece))

    def whole(block, half):
        return occ.at[block, half, pl.ds(0, nr)]

    if nr < ip:
        for block in range(cols):
            for half in range(2):
                occ[block, half, nr:ip] = jnp.zeros((ip - nr, wh), BF16)

    half_copy(grp, 0).start()
    vir_copy = pltpu.make_async_copy(vir_hbm, vraw, loc_sem.at[2])
    vir_copy.start()
    half_copy(other, 1).start()

    def h_copy(n, act):
        p, b, slot = n // nb, n % nb, n % 2
        last = ni - (nb - 1) * hb

        def go(size):
            copy = pltpu.make_async_copy(
                h_hbm.at[p, pl.ds(pl.multiple_of(b * hb, hb), size)], hbuf.at[slot, pl.ds(0, size)], h_sem.at[slot]
            )
            act(copy)

        if nb == 1:
            act(pltpu.make_async_copy(h_hbm.at[p], hbuf.at[slot], h_sem.at[slot]))
        elif last == hb:
            go(hb)
        else:
            pl.when(b < nb - 1)(lambda: go(hb))
            pl.when(b == nb - 1)(lambda: go(last))

    h_copy(jnp.int32(0), lambda c: c.start())
    pl.semaphore_wait(barrier, rows + cols - 1)

    def vir_send(block, target, n):
        return pltpu.make_async_remote_copy(
            src_ref=virt.at[block], dst_ref=virt.at[block], send_sem=vs_sem.at[n], recv_sem=vr_sem.at[block],
            device_id={"row": target}, device_id_type=MESH,
        )

    top = rows // 2

    def z_send(block, q, target, way):
        ref = occ.at[block, grp, rows_of(q)]
        return pltpu.make_async_remote_copy(
            src_ref=ref, dst_ref=ref, send_sem=zs_sem.at[way, block], recv_sem=zr_sem.at[block, q],
            device_id={"col": target}, device_id_type=MESH,
        )

    def y_send(block, q):
        ref = occ.at[block, grp, rows_of(q)]
        return pltpu.make_async_remote_copy(
            src_ref=ref, dst_ref=ref, send_sem=ys_sem.at[block], recv_sem=yr_sem.at[block],
            device_id={"grp": other}, device_id_type=MESH,
        )

    half_copy(grp, 0).wait()
    for q in range(PIECES):
        pl.when(col >= 1)(lambda q=q: z_send(col, q, col - 1, 0).start())
        pl.when(col <= cols - 2)(lambda q=q: z_send(col, q, col + 1, 1).start())

    vir_copy.wait()
    size = virt.shape[1]
    unit = lax.broadcasted_iota(jnp.int32, (size, size), 0) == lax.broadcasted_iota(jnp.int32, (size, size), 1)
    turned = lax.dot_general(unit.astype(F32).astype(BF16), vraw[...], NT, preferred_element_type=F32)
    virt[row] = turned.astype(BF16)
    vir_send(row, flip(row, top), 0).start()

    def forward(slot, q):
        def to_right():
            z_send(col - 1 - slot, q, col + 1, 1).start()

        def to_left():
            z_send(col + 1 + slot, q, col - 1, 0).start()

        pl.when((col - 1 - slot >= 0) & (col <= cols - 2))(to_right)
        pl.when((col + 1 + slot <= cols - 1) & (col >= 1))(to_left)

    def pump(slot, q):
        def from_left():
            block = col - 1 - slot
            z_send(block, q, 0, 1).wait_recv()
            y_send(block, q).start()

        def from_right():
            block = col + 1 + slot
            z_send(block, q, 0, 0).wait_recv()
            y_send(block, q).start()

        pl.when(col - 1 - slot >= 0)(from_left)
        pl.when(col + 1 + slot <= cols - 1)(from_right)
        before = slot * PIECES + q - HELD
        if before >= 0 and before // PIECES <= cols - 3:
            forward(before // PIECES, before % PIECES)

    pump(0, 0)
    held, bit = [0], top
    while bit >= 1:
        if bit != top:
            for h_at, h in enumerate(held):
                vir_send(flip_all(row, h), flip(row, bit), len(held) - 1 + h_at).start()
        for h in held:
            vir_send(flip_all(row, h + bit), row, 0).wait_recv()
        held = held + [h + bit for h in held]
        bit //= 2
    virt_out = pltpu.make_async_copy(virt, virt_hbm, loc_sem.at[2])
    virt_out.start()
    if PIECES > 1:
        pump(0, 1)

    steps = pert * nb

    def image_step(n, carry):
        pl.when(n + 1 < steps)(lambda: h_copy(n + 1, lambda c: c.start()))
        h_copy(n, lambda c: c.wait())
        p, b, slot = n // nb, n % nb, n % 2
        lhs = virt[...].reshape(nv, virt.shape[2])
        value = lax.dot_general(lhs, hbuf[slot], NT, preferred_element_type=F32)
        basis = lax.broadcasted_iota(jnp.int32, (1, hb), 1) + b * hb
        value = jnp.where(basis < ni, value, 0.0).astype(BF16)
        at = pl.ds(pl.multiple_of(p * nv, nv), nv)
        if nb == 1:
            image[at, :] = jnp.zeros((nv, ip), BF16)
            image[at, 0:hb] = value
        else:
            image[at, pl.ds(pl.multiple_of(b * hb, hb), hb)] = value
        for q in range(2, PIECES):
            at = min(steps - 1, (q - 1) * steps // (PIECES - 1))
            pl.when(n == at)(lambda q=q: pump(0, q))
        return carry

    lax.fori_loop(0, steps, image_step, 0)
    half_copy(other, 1).wait()

    order = [arrivals(cols, position) for position in range(cols)]

    def chunk(s):
        block = pick(col, [order[position][s][0] for position in range(cols)])
        second = pick(col, [order[position][s][1] for position in range(cols)])
        half = grp * (1 - second) + other * second
        return block, second, half

    def rs1_send(block, half, d, target):
        return pltpu.make_async_remote_copy(
            src_ref=part.at[block, half, target], dst_ref=rs1.at[block, half, d - 1],
            send_sem=a_s.at[block, half], recv_sem=a_r.at[block, half],
            device_id={"row": target}, device_id_type=MESH,
        )

    def make_part(s):
        block, second, half = chunk(s)
        if s >= 2:
            def await_second():
                pltpu.make_async_copy(whole(block, half), whole(block, half), yr_sem.at[block]).wait()
            pl.when(second == 1)(await_second)

        def body(d, carry):
            target = (row + d) % rows
            lhs = image[pl.ds(pl.multiple_of(target * pr, pr), pr), :]
            value = lax.dot_general(lhs, occ[block, half], NN, preferred_element_type=F32)
            part[block, half, target] = value.astype(BF16)
            pl.when(d < rows)(lambda: rs1_send(block, half, d, target).start())
            return carry

        lax.fori_loop(1, rows + 1, body, 0)

    def rs2_send(block, half, e):
        target = (col + e) % cols
        return pltpu.make_async_remote_copy(
            src_ref=rs2s.at[block, half, target], dst_ref=rs2r.at[block, half, e - 1],
            send_sem=b_s.at[block, half], recv_sem=b_r.at[block, half],
            device_id={"col": target}, device_id_type=MESH,
        )

    def combine(s):
        block, second, half = chunk(s)
        pltpu.make_async_copy(rs1.at[block, half], rs1.at[block, half], a_r.at[block, half]).wait()
        total = part[block, half, row].astype(F32)
        for d in range(rows - 1):
            total = total + rs1[block, half, d].astype(F32)
        rs2s[block, half] = total.reshape(cols, ps, wh).astype(BF16)
        for e in range(1, cols):
            rs2_send(block, half, e).start()

    def pair(d, second):
        half = grp if second == 0 else other
        return [(cols // 2 - 1 - d, half), (cols // 2 + d, half)]

    def ag1_send(block, half, e):
        ref = resp.at[block, half, row, col]
        return pltpu.make_async_remote_copy(
            src_ref=ref, dst_ref=ref, send_sem=c_s.at[block, half], recv_sem=c_r.at[block, half],
            device_id={"col": (col + e) % cols}, device_id_type=MESH,
        )

    def ag2_send(block, half, owner, target, n):
        ref = resp.at[block, half, owner]
        return pltpu.make_async_remote_copy(
            src_ref=ref, dst_ref=ref, send_sem=d_s.at[block, half], recv_sem=d_r.at[block, half, n],
            device_id={"row": target}, device_id_type=MESH,
        )

    def respond(d, second):
        for block, half in pair(d, second):
            pltpu.make_async_copy(rs2r.at[block, half], rs2r.at[block, half], b_r.at[block, half]).wait()
            total = rs2s[block, half, col].astype(F32)
            for e in range(cols - 1):
                total = total + rs2r[block, half, e].astype(F32)
            state = (row * pr + col * ps) % nv + lax.broadcasted_iota(jnp.int32, (ps, nv), 0)
            lane = lax.broadcasted_iota(jnp.int32, (ps, nv), 1)
            levels = jnp.sum(jnp.where(lane == state, vir_e[...], 0.0), axis=1, keepdims=True)
            gaps = occ_e[block, half] - levels
            resp[block, half, row, col] = (total / gaps).astype(BF16)
            for e in range(1, cols):
                ag1_send(block, half, e).start()

    def spread(d, second):
        for block, half in pair(d, second):
            some = resp.at[block, half, row, pl.ds(0, cols - 1)]
            pltpu.make_async_copy(some, some, c_r.at[block, half]).wait()
            ag2_send(block, half, row, flip(row, top), 0).start()
            if top > 1:
                ag2_send(block, half, row, flip(row, 1), rows - 2).start()

    def relay(d, second):
        held, bit, base = [0], top, 0
        while bit >= 1:
            for block, half in pair(d, second):
                for n, h in enumerate(held):
                    early = h == 0 and (bit == top or bit == 1)
                    if not early:
                        place = base + n if bit > 1 or n > 0 else rows - 2
                        place = base + n - 1 if bit == 1 and top > 1 else place
                        ag2_send(block, half, flip_all(row, h), flip(row, bit), place).start()
            for block, half in pair(d, second):
                for n in range(len(held)):
                    ag2_send(block, half, row, row, base + n).wait_recv()
            base += len(held)
            held = held + [h + bit for h in held]
            bit //= 2

    tile = dims["tile"]
    tiles = ip // tile

    def out_copy(n, slot):
        return [
            pltpu.make_async_copy(
                stage.at[slot, p], mixed_hbm.at[p, pl.ds(pl.multiple_of(n * tile, tile), tile)], o_sem.at[slot]
            )
            for p in range(pert)
        ]

    def mix(d, second, first, last):
        chunks = pair(d, second)

        def body(n, carry):
            at = pl.ds(pl.multiple_of(n * tile, tile), tile)
            if last:
                def free():
                    for copy in out_copy(n - 2, n % 2):
                        copy.wait()
                pl.when(n >= 2)(free)
            for p in range(pert):
                across = rows // pert
                total = None
                for block, half in chunks:
                    rhs = resp[block, half, pl.ds(p * across, across)]
                    rhs = rhs.astype(F32).reshape(nv, wh).astype(BF16)
                    value = lax.dot_general(occ[block, half, at], rhs, NT, preferred_element_type=F32)
                    total = value if total is None else total + value
                if not first:
                    total = total + acc[p, at]
                if last:
                    stage[n % 2, p] = total.astype(BF16)
                else:
                    acc[p, at] = total
            if last:
                for copy in out_copy(n, n % 2):
                    copy.start()
            return carry

        lax.fori_loop(0, tiles, body, 0)
        if last:
            for n in range(max(0, tiles - 2), tiles):
                for copy in out_copy(n, n % 2):
                    copy.wait()

    left = [(t, q) for t in range(1, cols - 1) for q in range(PIECES)]

    def through(slot):
        while left and left[0][0] <= slot:
            pump(*left.pop(0))

    def some_pumps(count, slot):
        for _ in range(count):
            if left and left[0][0] <= slot:
                pump(*left.pop(0))

    make_part(0)
    make_part(1)
    combine(0)
    make_part(2)
    combine(1)
    some_pumps(2, 1)
    make_part(3)
    combine(2)
    some_pumps(1, 1)
    combine(3)
    through(1)
    for s in range(4, cols):
        through((s - 2) // 2)
        make_part(s)
        some_pumps(1, (s - 2) // 2 + 1)
        combine(s)
    through((cols - 2) // 2)
    make_part(cols)
    combine(cols)
    some_pumps(1, cols // 2)
    make_part(cols + 1)
    respond(0, 0)
    some_pumps(1, cols // 2)
    combine(cols + 1)
    spread(0, 0)
    some_pumps(1, cols // 2)
    respond(0, 1)
    pairs = cols // 2
    for d in range(pairs - 1):
        s = cols + 2 * d + 2
        through((s - 2) // 2)
        make_part(s)
        relay(d, 0)
        spread(d, 1)
        some_pumps(1, s // 2)
        combine(s)
        mix(d, 0, d == 0, False)
        some_pumps(1, s // 2)
        relay(d, 1)
        make_part(s + 1)
        respond(d + 1, 0)
        some_pumps(1, s // 2)
        mix(d, 1, False, False)
        combine(s + 1)
        spread(d + 1, 0)
        some_pumps(1, s // 2)
        respond(d + 1, 1)
    relay(pairs - 1, 0)
    spread(pairs - 1, 1)
    mix(pairs - 1, 0, pairs == 1, False)
    relay(pairs - 1, 1)
    mix(pairs - 1, 1, False, True)

    virt_out.wait()
    for n in range(rows - 1):
        vir_send(row, row, n).wait_send()
    for block in range(cols):
        def sent(sem, ref=whole(block, 0)):
            pltpu.make_async_copy(ref, ref, sem).wait()

        pl.when((col >= 1) & (col <= block))(lambda: sent(zs_sem.at[0, block]))
        pl.when((col <= cols - 2) & (col >= block))(lambda: sent(zs_sem.at[1, block]))
        pl.when(col != block)(lambda: sent(ys_sem.at[block]))
        for half in range(2):
            sizes = (
                (a_s, rs1.at[block, half]),
                (b_s, rs2r.at[block, half]),
                (c_s, resp.at[block, half, 0, pl.ds(0, cols - 1)]),
                (d_s, resp.at[block, half, pl.ds(0, rows - 1)]),
            )
            for sem, ref in sizes:
                pltpu.make_async_copy(ref, ref, sem.at[block, half]).wait()


def flip_all(index, mask):
    bit = 1
    while bit <= mask:
        if mask & bit:
            index = flip(index, bit)
        bit *= 2
    return index


def final_kernel(mixed_ref, virt_ref, out_ref):
    out_ref[0] = lax.dot_general(mixed_ref[0], virt_ref[...], NN, preferred_element_type=F32).astype(BF16)


def per_device(mesh, perturbation, occ_coeffs, vir_coeffs, occ_energies, vir_energies):
    rows, cols = mesh.shape["row"], mesh.shape["col"]
    pert, ni, nj = perturbation.shape
    width = occ_coeffs.shape[1]
    nv = vir_coeffs.shape[1] * rows
    wh = up(-(-width // 2), 128)
    piece = up(-(-ni // PIECES), 64)
    ip = piece * PIECES
    hb = 512 if ni % 8 == 0 and ni > 512 else ni
    nb = -(-ni // hb)
    ip = up(max(nb * hb, ip), 256)
    piece = ip // PIECES
    pv = pert * nv
    pr = pv // rows
    ps = pr // cols
    tile = 512 if ip % 512 == 0 else 256
    dims = dict(rows=rows, cols=cols, pert=pert, ni=ni, hb=hb, nb=nb, nv=nv, ip=ip, piece=piece, wh=wh, tile=tile, nr=up(ni, 16))

    occ_padded = jnp.pad(occ_coeffs, ((0, up(ni, 16) - ni), (0, 2 * wh - width)))
    occ_e = jnp.pad(occ_energies.reshape(cols, width), ((0, 0), (0, 2 * wh - width)), constant_values=-1.0)
    occ_e = occ_e.reshape(cols, 2, 1, wh)
    vir_e = vir_energies[None, :]

    any_space = pl.BlockSpec(memory_space=pl.ANY)
    vmem = pl.BlockSpec(memory_space=pltpu.VMEM)
    dma = pltpu.SemaphoreType.DMA
    mixed, virt = pl.pallas_call(
        functools.partial(gather_kernel, dims),
        out_shape=(
            jax.ShapeDtypeStruct((pert, ip, nv), BF16),
            jax.ShapeDtypeStruct((rows, nv // rows, nj), BF16),
        ),
        in_specs=[any_space, any_space, any_space, vmem, vmem],
        out_specs=(any_space, any_space),
        scratch_shapes=[
            pltpu.VMEM((cols, 2, ip, wh), BF16),
            pltpu.VMEM((rows, nv // rows, nj), BF16),
            pltpu.VMEM((2, hb, nj), BF16),
            pltpu.VMEM((pv, ip), BF16),
            pltpu.VMEM((cols, 2, rows, pr, wh), BF16),
            pltpu.VMEM((cols, 2, rows - 1, pr, wh), BF16),
            pltpu.VMEM((cols, 2, cols, ps, wh), BF16),
            pltpu.VMEM((cols, 2, cols - 1, ps, wh), BF16),
            pltpu.VMEM((cols, 2, rows, cols, ps, wh), BF16),
            pltpu.VMEM((pert, ip, nv), F32),
            pltpu.VMEM((2, pert, tile, nv), BF16),
            pltpu.VMEM((nj, nv // rows), BF16),
            dma((3,)), dma((2,)), dma((rows,)), dma((rows,)),
            dma((2, cols)), dma((cols, PIECES)), dma((cols,)), dma((cols,)),
            dma((cols, 2)), dma((cols, 2)), dma((cols, 2)), dma((cols, 2)),
            dma((cols, 2)), dma((cols, 2)), dma((cols, 2)), dma((cols, 2, rows - 1)),
            dma((2,)),
        ],
        compiler_params=pltpu.CompilerParams(
            collective_id=0, has_side_effects=True, vmem_limit_bytes=67043328
        ),
        name="gather",
    )(perturbation, occ_padded, vir_coeffs, occ_e, vir_e)

    virt = virt.reshape(nv, nj)
    block = 768 if ip % 768 == 0 else 256
    return pl.pallas_call(
        final_kernel,
        out_shape=jax.ShapeDtypeStruct((pert, ni, nj), BF16),
        grid=(pert, ip // block),
        in_specs=[
            pl.BlockSpec((1, block, nv), lambda p, i: (p, i, 0)),
            pl.BlockSpec((nv, nj), lambda p, i: (0, 0)),
        ],
        out_specs=pl.BlockSpec((1, block, nj), lambda p, i: (p, i, 0)),
        compiler_params=pltpu.CompilerParams(vmem_limit_bytes=56 * 1024 * 1024),
        name="final",
    )(mixed, virt)


def solution(mesh):
    placed = (P("grp", "row", "col"), P("row", "col"), P("col", "row"), P(), P())
    return jax.shard_map(
        functools.partial(per_device, mesh), mesh=mesh, in_specs=placed,
        out_specs=P("grp", "row", "col"), check_vma=False,
    )
```
